32 devices in a mesh: groups: 2 (over y), dp: 4 (over z), mp: 4 (over x, core).
Axes of the slice: x: 2, y: 2, z: 4, core: 2. Of those that a mesh axis runs over, the one named last changes fastest.
Arguments:
- hidden: bfloat16 [8, 8192], P(('groups', 'mp'), 'dp'), parts along dimension 0, may hold values from -530 to 530
- attention_gain: float32 [8192], P('dp'), may hold values from 0.25 to 1.75
- query_weight: bfloat16 [8192, 8192], P('dp', 'mp'), may hold values from -0.0625 to 0.0625
- key_projector: bfloat16 [8192, 1024], P('dp', 'mp'), may hold values from -0.0625 to 0.0625
- value_projector: bfloat16 [8192, 1024], P('dp', 'mp'), may hold values from -0.0625 to 0.0625
- out_weight: bfloat16 [8192, 8192], P('mp', 'dp'), may hold values from -0.1875 to 0.1875
- key_cache: bfloat16 [8, 8, 256, 128], P(('groups', 'dp'), 'mp'), parts along dimension 0, may hold values from -1230 to 1230
- earlier_value_cache: bfloat16 [8, 8, 256, 128], P(('groups', 'dp'), 'mp'), parts along dimension 0, may hold values from -6 to 6
- cached_length_per_row: int32 [8], P(('groups', 'dp')), parts along dimension 0, may hold values from 1 to 256
- final_gain: float32 [8192], replicated, may hold values from 0.25 to 1.75
- head_weight: bfloat16 [32000, 8192], P('dp', 'mp'), may hold values from -41 to 41
- draft_ids: int32 [8], P(('groups', 'mp')), parts along dimension 0, may hold values from 0 to 31999
Outputs:
- residual_out: bfloat16 [8, 8192], P(('groups', 'mp'), 'dp'), parts along dimension 0
- draft_logprob: float32 [8], P(('groups', 'mp')), parts along dimension 0
The draws below stay inside these ranges and needn't reach their ends.
There are 2 independent parts, one for each index of `groups`. The reference program is written for one: setup_inputs(seed, part) draws one part's arguments, and reference() takes and returns one part's arrays. A program takes and returns all parts, laid end to end along the dimension named above; an argument that names none is the same for every part. Nothing has to cross between parts.
All inputs are finite; a program needn't handle non-finite values.
Results may differ from the reference program's by a relative error of at most 0.0035.
Values may be sent and summed in bfloat16 or wider, within the bound.
A program may use at most 128 MiB of HBM per device.

```python
import math
import jax
import jax.numpy as jnp
from jax import lax

MODEL_WIDTH = 8192
QUERY_HEADS = 64
KEY_VALUE_HEADS = 8
HEAD_WIDTH = 128
VOCAB = 32000
CACHE_SLOTS = 256
SEQUENCE_COUNT = 4


def draw_hidden(key, part):
    residual_streams = jax.random.split(jax.random.fold_in(key, 11), 3)
    row_scale = jnp.exp(jax.random.uniform(residual_streams[1], (SEQUENCE_COUNT, 1), minval=math.log(0.5), maxval=math.log(5.0)))
    col_scale = jnp.exp(jax.random.uniform(residual_streams[2], (1, MODEL_WIDTH), minval=math.log(0.5), maxval=math.log(2.0)))
    position = jnp.arange(MODEL_WIDTH, dtype=jnp.float32)[None, :] / MODEL_WIDTH
    cache_entries = jax.random.truncated_normal(residual_streams[0], -6.0, 6.0, (SEQUENCE_COUNT, MODEL_WIDTH))
    return (cache_entries * row_scale * col_scale * 3.0 ** position).astype(jnp.bfloat16)


def draw_key_cache(key, part):
    residual_streams = jax.random.split(jax.random.fold_in(key, 23), 2)
    per_head_scale = jnp.exp(jax.random.uniform(residual_streams[1], (SEQUENCE_COUNT, KEY_VALUE_HEADS, 1, 1), minval=0.0, maxval=math.log(4.0)))
    cache_entries = jax.random.truncated_normal(residual_streams[0], -6.0, 6.0, (SEQUENCE_COUNT, KEY_VALUE_HEADS, CACHE_SLOTS, HEAD_WIDTH)) * per_head_scale
    return cache_entries.astype(jnp.bfloat16)


def draw_head_weight(key, part):
    residual_streams = jax.random.split(jax.random.fold_in(key, 37), 2)
    position = jnp.arange(VOCAB, dtype=jnp.float32)[:, None] / VOCAB
    row_scale = jnp.exp(jax.random.uniform(residual_streams[1], (VOCAB, 1), minval=math.log(0.5), maxval=math.log(5.0)))
    row_scale = row_scale * 3.0 ** position / math.sqrt(MODEL_WIDTH)
    cache_entries = jax.random.truncated_normal(residual_streams[0], -6.0, 6.0, (VOCAB, MODEL_WIDTH)) * row_scale
    return cache_entries.astype(jnp.bfloat16)


def set_ends(values, key, smallest, largest):
    shape = values.shape
    spot = [jax.random.randint(jax.random.fold_in(key, axis), (), 0, shape[axis]) for axis in range(len(shape))]
    values = values.at[tuple(spot)].set(smallest)
    longest = shape.index(max(shape))
    spot[longest] = (spot[longest] + 1) % shape[longest]
    return values.at[tuple(spot)].set(largest)


def steps_of(stream_key, shape, cuts, smallest, top_value):
    def one(dim, shards_of):
        draws = jax.random.uniform(jax.random.fold_in(jax.random.fold_in(stream_key, 6), dim), (shards_of,), jnp.float32, smallest / len(cuts), top_value / len(cuts))
        return jnp.repeat(jnp.exp(draws), shape[dim] // shards_of).reshape((-1,) + (1,) * (len(shape) - dim - 1))

    loudness = one(*cuts[0])
    for cut in cuts[1:]:
        loudness = loudness * one(*cut)
    return loudness


def noise(rng, dims, deviation, limit, pieces=(), kind=jnp.bfloat16):
    level = steps_of(rng, dims, pieces, -0.22, 0.18) if pieces else 1.0
    values = jax.random.normal(rng, dims, jnp.float32) * deviation * level
    return jnp.minimum(jnp.maximum(values, -limit), limit).astype(kind)


def setup_inputs(seed: int = 0, part: int = 0) -> dict:
    streams_of = jax.random.split(jax.random.key(seed), 13)
    part_splits = jax.random.split(jax.random.fold_in(streams_of[12], part), 13)
    hidden = draw_hidden(jax.random.fold_in(jax.random.fold_in(streams_of[12], part), 71), part)
    attention_gain = jnp.clip(1.0 + 0.15 * jax.random.normal(streams_of[1], (MODEL_WIDTH,), jnp.float32), 0.25, 1.75)
    query_weight = noise(streams_of[2], (MODEL_WIDTH, QUERY_HEADS * HEAD_WIDTH), MODEL_WIDTH ** -0.5, 0.0625, ((0, 4), (1, 4)))
    key_projector = noise(streams_of[3], (MODEL_WIDTH, KEY_VALUE_HEADS * HEAD_WIDTH), MODEL_WIDTH ** -0.5, 0.0625, ((0, 4), (1, 4)))
    value_projector = noise(streams_of[4], (MODEL_WIDTH, KEY_VALUE_HEADS * HEAD_WIDTH), MODEL_WIDTH ** -0.5, 0.0625, ((0, 4), (1, 4)))
    out_weight = noise(streams_of[5], (QUERY_HEADS * HEAD_WIDTH, MODEL_WIDTH), (QUERY_HEADS * HEAD_WIDTH // 9) ** -0.5, 0.1875, ((0, 4), (1, 4)))
    key_cache = draw_key_cache(jax.random.fold_in(jax.random.fold_in(streams_of[12], part), 71), part)
    earlier_value_cache = noise(part_splits[7], (SEQUENCE_COUNT, KEY_VALUE_HEADS, CACHE_SLOTS, HEAD_WIDTH), 1.0, 6.0, ((0, 4), (1, 4)))
    cached_length_per_row = set_ends(jax.random.randint(part_splits[8], (SEQUENCE_COUNT,), 1, CACHE_SLOTS + 1), jax.random.fold_in(part_splits[8], 1), 1, CACHE_SLOTS).astype(jnp.int32)
    final_gain = jnp.clip(1.0 + 0.15 * jax.random.normal(streams_of[9], (MODEL_WIDTH,), jnp.float32), 0.25, 1.75)
    head_weight = draw_head_weight(jax.random.fold_in(streams_of[12], 71), part)
    draft_ids = set_ends(jax.random.randint(part_splits[11], (SEQUENCE_COUNT,), 0, VOCAB), jax.random.fold_in(part_splits[11], 1), 0, VOCAB - 1).astype(jnp.int32)
    return dict(hidden=hidden, attention_gain=attention_gain, query_weight=query_weight, key_projector=key_projector, value_projector=value_projector, out_weight=out_weight, key_cache=key_cache, earlier_value_cache=earlier_value_cache, cached_length_per_row=cached_length_per_row, final_gain=final_gain, head_weight=head_weight, draft_ids=draft_ids)


EPSILON = 1e-05
THETA = 10000.0

def rotary_embedding(vectors, positions):
    half_dim = vectors.shape[-1] // 2
    frequency = THETA ** (-2.0 * jnp.arange(half_dim, dtype=jnp.float32) / vectors.shape[-1])
    angles = positions.astype(jnp.float32)[:, None, None] * frequency[None, None, :]
    cosine = jnp.cos(angles)
    sine_part = jnp.sin(angles)
    former = vectors[..., :half_dim]
    latter = vectors[..., half_dim:]
    return jnp.concatenate([former * cosine - latter * sine_part, latter * cosine + former * sine_part], axis=-1)

def rms_normed(matrix, gain_row):
    wide_rows = matrix.astype(jnp.float32)
    mean_square = lax.optimization_barrier(jnp.mean(wide_rows * wide_rows, axis=-1, keepdims=True))
    return (wide_rows * lax.rsqrt(mean_square + EPSILON) * gain_row).astype(jnp.bfloat16)

def attend(query_rows, key_cache, earlier_value_cache, incoming_key, incoming_value, lengths):
    score_scale = HEAD_WIDTH ** (-0.5)
    scores = jnp.einsum('bgrd,bgtd->bgrt', query_rows.astype(jnp.float32), key_cache.astype(jnp.float32)) * score_scale
    places = lax.broadcasted_iota(jnp.int32, scores.shape, 3)
    scores = jnp.where(places < lengths[:, None, None, None], scores, -jnp.inf)
    own_score = jnp.einsum('bgrd,bgd->bgr', query_rows.astype(jnp.float32), incoming_key.astype(jnp.float32)) * score_scale
    highest = jnp.maximum(lax.optimization_barrier(jnp.max(scores, axis=3)), own_score)
    exponent = jnp.exp(scores - highest[..., None])
    own_exp = jnp.exp(own_score - highest)
    denominator = lax.optimization_barrier(jnp.sum(exponent, axis=3)) + own_exp
    weights = lax.optimization_barrier(exponent.astype(jnp.bfloat16)).astype(jnp.float32)
    own_weight = lax.optimization_barrier(own_exp.astype(jnp.bfloat16)).astype(jnp.float32)
    numerator = jnp.einsum('bgrt,bgtd->bgrd', weights, earlier_value_cache.astype(jnp.float32))
    numerator = numerator + own_weight[..., None] * incoming_value.astype(jnp.float32)[:, :, None, :]
    return (numerator / denominator[..., None]).astype(jnp.bfloat16)

def reference(hidden, attention_gain, query_weight, key_projector, value_projector, out_weight, key_cache, earlier_value_cache, cached_length_per_row, final_gain, head_weight, draft_ids):
    normed_in = rms_normed(hidden, attention_gain)
    query_raw = jnp.dot(normed_in, query_weight, preferred_element_type=jnp.float32)
    unrotated_key = jnp.dot(normed_in, key_projector, preferred_element_type=jnp.float32)
    projected_value = jnp.dot(normed_in, value_projector, preferred_element_type=jnp.float32)
    query_rows = rotary_embedding(query_raw.reshape(SEQUENCE_COUNT, QUERY_HEADS, HEAD_WIDTH), cached_length_per_row).astype(jnp.bfloat16)
    query_rows = query_rows.reshape(SEQUENCE_COUNT, KEY_VALUE_HEADS, QUERY_HEADS // KEY_VALUE_HEADS, HEAD_WIDTH)
    incoming_key = rotary_embedding(unrotated_key.reshape(SEQUENCE_COUNT, KEY_VALUE_HEADS, HEAD_WIDTH), cached_length_per_row).astype(jnp.bfloat16)
    incoming_value = projected_value.reshape(SEQUENCE_COUNT, KEY_VALUE_HEADS, HEAD_WIDTH).astype(jnp.bfloat16)
    mixed = attend(query_rows, key_cache, earlier_value_cache, incoming_key, incoming_value, cached_length_per_row).reshape(SEQUENCE_COUNT, QUERY_HEADS * HEAD_WIDTH)
    attention_out = jnp.dot(mixed, out_weight, preferred_element_type=jnp.float32)
    residual_out = (hidden.astype(jnp.float32) + attention_out).astype(jnp.bfloat16)
    normed_out = rms_normed(residual_out, final_gain)
    logits = jnp.dot(normed_out, head_weight.T, preferred_element_type=jnp.float32)
    highest = lax.optimization_barrier(jnp.max(logits, axis=1))
    log_total = highest + jnp.log(lax.optimization_barrier(jnp.sum(jnp.exp(logits - highest[:, None]), axis=1)))
    target_logit = jnp.take_along_axis(logits, draft_ids[:, None].astype(jnp.int32), axis=1)[:, 0]
    return (residual_out, target_logit - log_total)
```

```python
import functools
import math

import jax
import jax.numpy as jnp
from jax import lax
from jax.experimental import pallas as pl
from jax.experimental.pallas import tpu as pltpu
from jax.sharding import PartitionSpec as P

EPSILON = 1e-05
THETA = 10000.0
LANES = 128
MESH = pl.DeviceIdType.MESH
F32 = jnp.float32
BF16 = jnp.bfloat16


def each(first, last, body):
    if last - first <= 16:
        for k in range(first, last):
            body(k)
    else:

        @pl.loop(first, last)
        def _(k):
            body(k)


def aligned(start):
    return start if isinstance(start, int) else pl.multiple_of(start, LANES)


def kernel(
    n_dp, n_mp, chunk,
    hidden, attention_gain, query_weight, key_projector, value_projector, out_weight,
    key_cache, value_cache, lengths, final_gain, head_weight, draft_ids,
    residual_out, logprob_out,
    hid_v, gain_v, wq_v, wk_v, wv_v, wo_v, kc_v, vc_v, fgain_v, head_v,
    x_recv, x_v, ss_send, ss_recv, proj_send, proj_recv, mix_send, mix_recv, mix_v,
    att_send, att_recv, res_send, res_recv, ss2_send, ss2_recv, y_v,
    log_send, log_recv, fin_send, fin_recv,
    load_sem, head_sem, out_sem,
    x_ss, x_rs, ss_ss, ss_rs, proj_ss, proj_rs, mix_ss, mix_rs, att_ss, att_rs,
    res_ss, res_rs, ss2_ss, ss2_rs, log_ss, log_rs, fin_ss, fin_rs,
):
    j = lax.axis_index("dp")
    i = lax.axis_index("mp")
    count = n_dp * n_mp
    me = j * n_mp + i
    rows, width = hid_v.shape
    total_rows = rows * n_mp
    model_width = width * n_dp
    sequences, pairs, slots, head_size = kc_v.shape
    query_cols = wq_v.shape[1]
    pair_cols = wk_v.shape[1]
    group = query_cols // pair_cols
    quarter = y_v.shape[1]
    blocks = quarter // width
    vocab = head_v.shape[0]
    chunks = log_send.shape[0]
    full = vocab // chunk

    def load(source, target, slot):
        copy = pltpu.make_async_copy(source, target, load_sem.at[slot])
        copy.start()
        return copy

    hid_in = load(hidden, hid_v, 0)
    gain_in = load(attention_gain, gain_v, 1)
    wk_in = load(key_projector, wk_v, 2)
    wv_in = load(value_projector, wv_v, 3)
    wq_in = load(query_weight, wq_v, 4)
    kc_in = load(key_cache, kc_v, 5)
    vc_in = load(value_cache, vc_v, 6)
    wo_in = load(out_weight, wo_v, 7)
    fgain_in = load(final_gain.at[:, pl.ds(pl.multiple_of(i * quarter, LANES), quarter)], fgain_v, 8)

    def head_copy(c):
        size = chunk if c < full else vocab - full * chunk
        return pltpu.make_async_copy(
            head_weight.at[pl.ds(c * chunk, size)], head_v.at[pl.ds(c * chunk, size)], head_sem.at[c]
        )

    for c in range(chunks):
        head_copy(c).start()

    def place(number):
        return {"dp": number // n_mp, "mp": lax.rem(number, n_mp)}

    barrier = pltpu.get_barrier_semaphore()

    def greet(k):
        pl.semaphore_signal(
            barrier, inc=1, device_id=place(lax.rem(me + k, count)), device_id_type=MESH
        )

    each(1, count, greet)

    def remote(source, target, send, receive, device):
        return pltpu.make_async_remote_copy(
            src_ref=source, dst_ref=target, send_sem=send, recv_sem=receive,
            device_id=device, device_id_type=MESH,
        )

    hid_in.wait()
    own = hid_v[...].astype(F32)
    ss_send[...] = jnp.broadcast_to(jnp.sum(own * own, axis=1, keepdims=True), ss_send.shape)
    ss_recv[me] = ss_send[...]
    x_recv[i] = hid_v[...]

    lane = lax.broadcasted_iota(jnp.int32, (1, head_size), 1)
    half = head_size // 2
    index = jnp.where(lane < half, lane, lane - half).astype(F32)
    frequency = jnp.exp(index * (-2.0 * math.log(THETA) / head_size))
    turns = []
    for s in range(sequences):
        angles = lengths[s].astype(F32) * frequency
        sine = jnp.sin(angles)
        turns.append((jnp.cos(angles), jnp.where(lane < half, -sine, sine)))

    pl.semaphore_wait(barrier, count - 1)

    def x_copy(k):
        return remote(
            hid_v, x_recv.at[i], x_ss.at[k], x_rs.at[i], {"dp": j, "mp": lax.rem(i + k, n_mp)}
        )

    def ss_copy(k):
        return remote(
            ss_send, ss_recv.at[me], ss_ss.at[k], ss_rs.at[me], place(lax.rem(me + k, count))
        )

    each(1, count, lambda k: ss_copy(k).start())
    each(1, n_mp, lambda k: x_copy(k).start())

    def arrived(n, mine, buffer, sems):
        def one(k):
            source = lax.rem(mine + k, n)
            pltpu.make_async_copy(buffer.at[source], buffer.at[source], sems.at[source]).wait()

        each(1, n, one)

    def row_scales(buffer):
        scales = []
        for r in range(n_mp):
            squares = buffer[r]
            for d in range(1, n_dp):
                squares += buffer[d * n_mp + r]
            scales.append(lax.rsqrt(squares[:, :1] / model_width + EPSILON))
        return scales

    gain_in.wait()
    arrived(n_mp, i, x_recv, x_rs)
    arrived(count, me, ss_recv, ss_rs)
    scales = row_scales(ss_recv)
    gain = gain_v[...]
    x_v[...] = jnp.concatenate(
        [x_recv[r].astype(F32) * scales[r] * gain for r in range(n_mp)], axis=0
    ).astype(BF16)

    def project(left, weight, keep, base, parts, size):
        columns = weight.shape[1]
        step = min(512, columns)

        def one(c):
            start = aligned(c * step)
            part = jnp.dot(left[...], weight[:, pl.ds(start, step)], preferred_element_type=F32)
            for t in range(parts):
                keep[t, :, pl.ds(aligned(base + start), step)] = part[t * size : (t + 1) * size]

        if columns == step:
            one(0)
        else:

            @pl.loop(0, columns // step)
            def _(c):
                one(c)

    wk_in.wait()
    project(x_v, wk_v, proj_send, query_cols, n_dp, sequences)
    wv_in.wait()
    project(x_v, wv_v, proj_send, query_cols + pair_cols, n_dp, sequences)
    wq_in.wait()
    project(x_v, wq_v, proj_send, 0, n_dp, sequences)

    def proj_copy(k):
        t = lax.rem(j + k, n_dp)
        return remote(
            proj_send.at[t], proj_recv.at[j], proj_ss.at[k], proj_rs.at[j], {"dp": t, "mp": i}
        )

    each(1, n_dp, lambda k: proj_copy(k).start())
    kc_in.wait()
    vc_in.wait()
    arrived(n_dp, j, proj_recv, proj_rs)
    proj_recv[j] = proj_send[j]
    projected = proj_recv[0]
    for d in range(1, n_dp):
        projected += proj_recv[d]

    def rotated(vectors, turn):
        swapped = jnp.concatenate([vectors[:, half:], vectors[:, :half]], axis=1)
        return (vectors * turn[0] + swapped * turn[1]).astype(BF16)

    scale = head_size ** (-0.5)
    for s in range(sequences):
        def heads_of(start, number):
            return jnp.concatenate(
                [
                    projected[s : s + 1, start + h * head_size : start + (h + 1) * head_size]
                    for h in range(number)
                ],
                axis=0,
            )

        queries = rotated(heads_of(0, pairs * group), turns[s])
        keys = rotated(heads_of(query_cols, pairs), turns[s])
        values = heads_of(query_cols + pair_cols, pairs).astype(BF16)
        mixed = []
        for g in range(pairs):
            query = queries[g * group : (g + 1) * group]
            own_score = scale * jnp.sum(
                query.astype(F32) * keys[g : g + 1].astype(F32), axis=1, keepdims=True
            )
            scores = scale * lax.dot_general(
                query, kc_v[s, g], (((1,), (1,)), ((), ())), preferred_element_type=F32
            )
            spots = lax.broadcasted_iota(jnp.int32, scores.shape, 1)
            scores = jnp.where(spots < lengths[s], scores, -jnp.inf)
            highest = jnp.maximum(jnp.max(scores, axis=1, keepdims=True), own_score)
            exponent = jnp.exp(scores - highest)
            own_exp = jnp.exp(own_score - highest)
            denominator = jnp.sum(exponent, axis=1, keepdims=True) + own_exp
            numerator = jnp.dot(exponent.astype(BF16), vc_v[s, g], preferred_element_type=F32)
            numerator += own_exp.astype(BF16).astype(F32) * values[g : g + 1].astype(F32)
            mixed.append(numerator / denominator)
        mixed = [m[h : h + 1] for m in mixed for h in range(group)]
        mix_send[s : s + 1] = jnp.concatenate(mixed, axis=1).astype(BF16)

    def mix_copy(k):
        return remote(
            mix_send, mix_recv.at[j], mix_ss.at[k], mix_rs.at[j],
            {"dp": lax.rem(j + k, n_dp), "mp": i},
        )

    each(1, n_dp, lambda k: mix_copy(k).start())
    mix_recv[j] = mix_send[...]
    wo_in.wait()
    arrived(n_dp, j, mix_recv, mix_rs)
    mix_v[...] = jnp.concatenate(
        [mix_recv[d].astype(F32) for d in range(n_dp)], axis=0
    ).astype(BF16)
    project(mix_v, wo_v, att_send, 0, n_mp, rows)

    def att_copy(k):
        t = lax.rem(i + k, n_mp)
        return remote(
            att_send.at[t], att_recv.at[i], att_ss.at[k], att_rs.at[i], {"dp": j, "mp": t}
        )

    each(1, n_mp, lambda k: att_copy(k).start())
    att_recv[i] = att_send[i]
    arrived(n_mp, i, att_recv, att_rs)
    attended = att_recv[0]
    for r in range(1, n_mp):
        attended += att_recv[r]
    residual = (hid_v[...].astype(F32) + attended).astype(BF16)
    res_send[...] = residual
    wide = residual.astype(F32)
    ss2_send[...] = jnp.broadcast_to(jnp.sum(wide * wide, axis=1, keepdims=True), ss2_send.shape)

    reader = j // blocks
    spot = lax.rem(j, blocks) * n_mp + i

    def res_copy(k):
        return remote(
            res_send, res_recv.at[spot], res_ss.at[k], res_rs.at[spot],
            {"dp": lax.rem(j + k, n_dp), "mp": reader},
        )

    def ss2_copy(k):
        return remote(
            ss2_send, ss2_recv.at[me], ss2_ss.at[k], ss2_rs.at[me], place(lax.rem(me + k, count))
        )

    each(1, n_dp, lambda k: res_copy(k).start())

    @pl.when(reader != i)
    def _():
        res_copy(0).start()

    @pl.when(reader == i)
    def _():
        res_recv[spot] = residual

    each(1, count, lambda k: ss2_copy(k).start())
    ss2_recv[me] = ss2_send[...]
    result = pltpu.make_async_copy(res_send, residual_out, out_sem)
    result.start()

    def res_wait(k):
        source = (i * blocks + k // n_mp) * n_mp + lax.rem(k, n_mp)

        @pl.when(source != me)
        def _():
            pltpu.make_async_copy(res_recv.at[k], res_recv.at[k], res_rs.at[k]).wait()

    each(0, blocks * n_mp, res_wait)
    fgain_in.wait()
    arrived(count, me, ss2_recv, ss2_rs)
    scales = row_scales(ss2_recv)
    y_v[...] = jnp.concatenate(
        [
            jnp.concatenate([res_recv[b * n_mp + r].astype(F32) for b in range(blocks)], axis=1)
            * scales[r]
            * fgain_v[...]
            for r in range(n_mp)
        ],
        axis=0,
    ).astype(BF16)

    def log_copy(c, k):
        t = lax.rem(i + k, n_mp)
        return remote(
            log_send.at[c, t], log_recv.at[c, i], log_ss.at[c * n_mp + k], log_rs.at[c * n_mp + i],
            {"dp": j, "mp": t},
        )

    def head_chunk(c, size):
        piece = 256
        for p in range(0, size, piece):
            wide_piece = min(piece, size - p)
            part = lax.dot_general(
                y_v[...], head_v[pl.ds(c * chunk + p, wide_piece)],
                (((1,), (1,)), ((), ())), preferred_element_type=F32,
            )
            for t in range(n_mp):
                log_send[c, t, :, p : p + wide_piece] = part[t * rows : (t + 1) * rows]
        each(1, n_mp, lambda k: log_copy(c, k).start())

    if full:

        @pl.loop(0, full)
        def _(c):
            start = pl.multiple_of(c * chunk, chunk)
            pltpu.make_async_copy(
                head_weight.at[pl.ds(start, chunk)], head_v.at[pl.ds(start, chunk)], head_sem.at[c]
            ).wait()
            head_chunk(c, chunk)

    if chunks > full:
        rest = vocab - full * chunk
        head_copy(full).wait()
        log_send[full, :, :, rest // LANES * LANES :] = jnp.zeros(
            (n_mp, rows, chunk - rest // LANES * LANES), F32
        )
        head_chunk(full, rest)

    ids = jnp.zeros((rows, 1), jnp.int32)
    row_index = lax.broadcasted_iota(jnp.int32, (rows, 1), 0)
    for r in range(rows):
        ids = jnp.where(row_index == r, draft_ids[r], ids)
    column = lax.broadcasted_iota(jnp.int32, (rows, chunk), 1)
    pieces = []
    target = jnp.zeros((rows, chunk), F32)
    for c in range(chunks):
        logits = log_send[c, i]
        for k in range(1, n_mp):
            source = lax.rem(i + k, n_mp)
            pltpu.make_async_copy(
                log_recv.at[c, source], log_recv.at[c, source], log_rs.at[c * n_mp + source]
            ).wait()
            logits += log_recv[c, source]
        if c >= full:
            logits = jnp.where(column < vocab - c * chunk, logits, -jnp.inf)
        target = jnp.where(column + (c * chunk + j * vocab) == ids, logits, target)
        pieces.append(logits)
    if chunks > full:
        inside = ids < (j + 1) * vocab
        target = jnp.where(inside, target, 0.0)
    peak = pieces[0]
    for piece in pieces[1:]:
        peak = jnp.maximum(peak, piece)
    peak = jnp.max(peak, axis=1, keepdims=True)
    mass = jnp.exp(pieces[0] - peak)
    for piece in pieces[1:]:
        mass += jnp.exp(piece - peak)
    mass = jnp.sum(mass, axis=1, keepdims=True)
    target = jnp.sum(target, axis=1, keepdims=True)
    lanes = lax.broadcasted_iota(jnp.int32, (rows, LANES), 1)
    fin_send[...] = jnp.where(lanes == 0, peak, jnp.where(lanes == 1, mass, target))

    def fin_copy(k):
        return remote(
            fin_send, fin_recv.at[j], fin_ss.at[k], fin_rs.at[j],
            {"dp": lax.rem(j + k, n_dp), "mp": i},
        )

    each(1, n_dp, lambda k: fin_copy(k).start())
    fin_recv[j] = fin_send[...]

    each(1, count, lambda k: ss_copy(k).wait_send())
    each(1, n_mp, lambda k: x_copy(k).wait_send())
    each(1, n_dp, lambda k: proj_copy(k).wait_send())
    each(1, n_dp, lambda k: mix_copy(k).wait_send())
    each(1, n_mp, lambda k: att_copy(k).wait_send())
    each(1, n_dp, lambda k: res_copy(k).wait_send())

    @pl.when(reader != i)
    def _():
        res_copy(0).wait_send()

    each(1, count, lambda k: ss2_copy(k).wait_send())
    for c in range(chunks):
        each(1, n_mp, lambda k: log_copy(c, k).wait_send())
    result.wait()
    arrived(n_dp, j, fin_recv, fin_rs)
    each(1, n_dp, lambda k: fin_copy(k).wait_send())

    tiles = [fin_recv[d] for d in range(n_dp)]
    overall = tiles[0][:, 0:1]
    for tile in tiles[1:]:
        overall = jnp.maximum(overall, tile[:, 0:1])
    mass = jnp.zeros_like(overall)
    target = jnp.zeros_like(overall)
    for tile in tiles:
        mass += tile[:, 1:2] * jnp.exp(tile[:, 0:1] - overall)
        target += tile[:, 2:3]
    logprob = target - (overall + jnp.log(mass))
    for r in range(rows):
        logprob_out[r] = logprob[r, 0]


def solution(mesh):
    n_dp, n_mp = mesh.shape["dp"], mesh.shape["mp"]

    def shards(
        hidden, attention_gain, query_weight, key_projector, value_projector, out_weight,
        key_cache, earlier_value_cache, cached_length_per_row, final_gain, head_weight, draft_ids,
    ):
        rows, width = hidden.shape
        sequences = key_cache.shape[0]
        query_cols = query_weight.shape[1]
        wide = query_cols + key_projector.shape[1] + value_projector.shape[1]
        vocab, quarter = head_weight.shape
        count = n_dp * n_mp
        chunk = min(1024, -(-vocab // LANES) * LANES)
        chunks = -(-vocab // chunk)
        blocks = quarter // width
        vmem, dma = pltpu.VMEM, pltpu.SemaphoreType.DMA
        flat = (1, width)
        scratch = [
            vmem(hidden.shape, BF16), vmem(flat, F32),
            *[vmem(w.shape, BF16) for w in (query_weight, key_projector, value_projector, out_weight)],
            vmem(key_cache.shape, BF16), vmem(earlier_value_cache.shape, BF16),
            vmem((1, quarter), F32), vmem(head_weight.shape, BF16),
            vmem((n_mp, rows, width), BF16), vmem((n_mp * rows, width), BF16),
            vmem((rows, LANES), F32), vmem((count, rows, LANES), F32),
            vmem((n_dp, sequences, wide), F32), vmem((n_dp, sequences, wide), F32),
            vmem((sequences, query_cols), BF16), vmem((n_dp, sequences, query_cols), BF16),
            vmem((n_dp * sequences, query_cols), BF16),
            vmem((n_mp, rows, width), F32), vmem((n_mp, rows, width), F32),
            vmem((rows, width), BF16), vmem((blocks * n_mp, rows, width), BF16),
            vmem((rows, LANES), F32), vmem((count, rows, LANES), F32),
            vmem((n_mp * rows, quarter), BF16),
            vmem((chunks, n_mp, rows, chunk), F32), vmem((chunks, n_mp, rows, chunk), F32),
            vmem((rows, LANES), F32), vmem((n_dp, rows, LANES), F32),
            dma((9,)), dma((chunks,)), dma,
            dma((n_mp,)), dma((n_mp,)), dma((count,)), dma((count,)),
            dma((n_dp,)), dma((n_dp,)), dma((n_dp,)), dma((n_dp,)), dma((n_mp,)), dma((n_mp,)),
            dma((n_dp,)), dma((blocks * n_mp,)), dma((count,)), dma((count,)),
            dma((chunks * n_mp,)), dma((chunks * n_mp,)), dma((n_dp,)), dma((n_dp,)),
        ]
        anywhere = pl.BlockSpec(memory_space=pl.ANY)
        scalars = pl.BlockSpec(memory_space=pltpu.SMEM)
        return pl.pallas_call(
            functools.partial(kernel, n_dp, n_mp, chunk),
            out_shape=(
                jax.ShapeDtypeStruct(hidden.shape, BF16),
                jax.ShapeDtypeStruct(draft_ids.shape, F32),
            ),
            in_specs=[anywhere] * 8 + [scalars] + [anywhere] * 2 + [scalars],
            out_specs=(anywhere, scalars),
            scratch_shapes=scratch,
            compiler_params=pltpu.CompilerParams(
                collective_id=0, has_side_effects=True, vmem_limit_bytes=67043328
            ),
        )(
            hidden, attention_gain.reshape(flat), query_weight, key_projector, value_projector,
            out_weight, key_cache, earlier_value_cache, cached_length_per_row,
            final_gain.reshape(1, -1), head_weight, draft_ids,
        )

    in_specs = (
        P(("groups", "mp"), "dp"),
        P("dp"),
        P("dp", "mp"),
        P("dp", "mp"),
        P("dp", "mp"),
        P("mp", "dp"),
        P(("groups", "dp"), "mp", None, None),
        P(("groups", "dp"), "mp", None, None),
        P(("groups", "dp")),
        P(),
        P("dp", "mp"),
        P(("groups", "mp")),
    )
    out_specs = (P(("groups", "mp"), "dp"), P(("groups", "mp")))
    return jax.shard_map(shards, mesh=mesh, in_specs=in_specs, out_specs=out_specs, check_vma=False)
```
